32 devices in a mesh: shift: 8 (over y, x, core), dom: 4 (over z).
Axes of the slice: x: 2, y: 2, z: 4, core: 2. Of those that a mesh axis runs over, the one named last changes fastest.
Arguments:
- samples: float32 [32, 64, 1024], P('dom'), may hold values from -6 to 6
- potential: float32 [32, 1024], P('dom'), may hold values from 0 to 4
Outputs:
- subspace: float32 [32, 64, 1024], P('dom')
- reduced_h: float32 [64, 64], replicated
- reduced_b: float32 [64, 64], replicated
The draws below stay inside these ranges and needn't reach their ends.
All inputs are finite; a program needn't handle non-finite values.
Results may differ from the reference program's by a relative error of at most 0.00027.
Values sent between devices are 32-bit elements; how exact they have to be, the bound alone decides.
A program may use at most 128 MiB of HBM per device.

```python
import math
import jax
import jax.numpy as jnp
from jax import lax

NV = 64
NX = 32
NY = 32
NZ = 32
NXY = 1024
SHIFTS = 8


def block_levels(stream_key, shape, cuts, least, high):
    loudness, own = 1.0, jax.random.fold_in(stream_key, 6)
    for axis_at, shards_of in cuts:
        steps = jnp.exp(jax.random.uniform(jax.random.fold_in(own, axis_at), (shards_of,), jnp.float32, least / len(cuts), high / len(cuts)))
        loudness = loudness * jnp.repeat(steps, shape[axis_at] // shards_of).reshape([-1 if axis == axis_at else 1 for axis in range(len(shape))])
    return loudness


def normal_values(key, shape, deviation, limit, shards=(), kind=jnp.bfloat16):
    entries = jax.random.normal(key, shape, jnp.float32) * deviation
    if len(shards) > 0:
        entries = block_levels(key, shape, shards, -0.22, 0.18) * entries
    return jnp.clip(entries, min=-limit, max=limit).astype(kind)


def setup_inputs(seed: int = 0) -> dict:
    splits = jax.random.split(jax.random.key(seed), 3)
    return {
        "samples": normal_values(splits[0], (NZ, NV, NXY), 1.0, 6.0, ((0, 4),), jnp.float32),
        "potential": jnp.clip(4.0 * jax.random.uniform(splits[1], (NZ, NXY), jnp.float32) ** block_levels(splits[1], (NZ, NXY), ((0, 4),), -0.2, 0.2), 0.0, 4.0),
    }


CENTRE = 3.0
RADIUS = 2.0
RIDGE = 0.01


def plane_sum(values):
    grid = values.reshape(values.shape[:-1] + (NX, NY))
    padded = jnp.pad(grid, [(0, 0)] * (values.ndim - 1) + [(1, 1), (1, 1)])
    total = padded[..., 2:, 1:-1] + padded[..., :-2, 1:-1] + padded[..., 1:-1, 2:] + padded[..., 1:-1, :-2]
    return total.reshape(values.shape)


def hamiltonian(values, onsite):
    padded = jnp.pad(values, [(1, 1)] + [(0, 0)] * (values.ndim - 1))
    return onsite * values - (padded[2:] + padded[:-2] + plane_sum(values))


def colsum(values):
    return jnp.sum(values, axis=(0, 2))


def reference(samples, potential):
    onsite = (6.0 + potential)[:, None, :]
    moment = jnp.zeros(samples.shape, jnp.float32)
    for order in range(SHIFTS):
        angle = math.pi * (order + 0.5) / SHIFTS
        shift_re = CENTRE + RADIUS * math.cos(angle)
        shift_im = RADIUS * math.sin(angle)
        weight_re = RADIUS * math.cos(angle) / SHIFTS
        weight_im = RADIUS * math.sin(angle) / SHIFTS
        diag_re = shift_re - onsite
        modulus = diag_re * diag_re + shift_im * shift_im
        inv_re = diag_re / modulus
        inv_im = -shift_im / modulus

        def preconditioning_operator(real_part, imag_part):
            return real_part * inv_re - imag_part * inv_im, real_part * inv_im + imag_part * inv_re

        def operate(real_part, imag_part):
            ham_re = hamiltonian(real_part, onsite)
            ham_im = hamiltonian(imag_part, onsite)
            return (shift_re * real_part - shift_im * imag_part - ham_re,
                    shift_re * imag_part + shift_im * real_part - ham_im)

        first_block_real, first_block_imag = operate(samples * inv_re, samples * inv_im)
        two_re, two_im = operate(*preconditioning_operator(first_block_real, first_block_imag))
        g_one = colsum(first_block_real * first_block_real + first_block_imag * first_block_imag)
        q_one_re = colsum(first_block_real * samples)
        q_one_im = colsum(-first_block_imag * samples)
        g_mix_re = colsum(first_block_real * two_re + first_block_imag * two_im)
        g_mix_im = colsum(first_block_real * two_im - first_block_imag * two_re)
        g_two = colsum(two_re * two_re + two_im * two_im)
        q_two_re = colsum(two_re * samples)
        q_two_im = colsum(-two_im * samples)
        ridge = RIDGE * (g_one + g_two) / 2.0
        determ = (g_one + ridge) * (g_two + ridge) - (g_mix_re * g_mix_re + g_mix_im * g_mix_im)
        coef_one_re = ((g_two + ridge) * q_one_re - (g_mix_re * q_two_re - g_mix_im * q_two_im)) / determ
        coef_one_im = ((g_two + ridge) * q_one_im - (g_mix_re * q_two_im + g_mix_im * q_two_re)) / determ
        coef_two_re = ((g_one + ridge) * q_two_re - (g_mix_re * q_one_re + g_mix_im * q_one_im)) / determ
        coefficient_second_imag = ((g_one + ridge) * q_two_im - (g_mix_re * q_one_im - g_mix_im * q_one_re)) / determ
        first_coefficient_real = coef_one_re[None, :, None]
        first_coefficient_imag = coef_one_im[None, :, None]
        second_coefficient_real = coef_two_re[None, :, None]
        second_coefficient_imag = coefficient_second_imag[None, :, None]
        solved_real_part, solved_imag_part = preconditioning_operator(first_coefficient_real * samples + second_coefficient_real * first_block_real - second_coefficient_imag * first_block_imag,
                                 first_coefficient_imag * samples + second_coefficient_real * first_block_imag + second_coefficient_imag * first_block_real)
        moment = moment + (weight_re * solved_real_part - weight_im * solved_imag_part)
    scale = 1.0 / (NX * NY * NZ)
    applied = hamiltonian(moment, onsite)
    reduced_h = jnp.einsum('znc,zmc->nm', moment, applied, precision=lax.Precision.HIGHEST) * scale
    reduced_b = jnp.einsum('znc,zmc->nm', moment, moment, precision=lax.Precision.HIGHEST) * scale
    return moment, reduced_h, reduced_b
```

```python
import functools
import math

import jax
import jax.numpy as jnp
from jax import lax
from jax.experimental import pallas as pl
from jax.experimental.pallas import tpu as pltpu
from jax.sharding import PartitionSpec as P

NX = 32
NY = 32
LANES = 128

CENTRE = 3.0
RADIUS = 2.0
RIDGE = 0.01
MESH = pl.DeviceIdType.MESH


def tiles_of(value):
    return [value[:, at : at + LANES] for at in range(0, value.shape[1], LANES)]


def plane_sum(value):
    tiles = tiles_of(value)
    lane = lax.broadcasted_iota(jnp.int32, tiles[0].shape, 1)
    column = lane % NY
    zero = jnp.zeros_like(tiles[0])
    out = []
    for at, tile in enumerate(tiles):
        before = tiles[at - 1] if at > 0 else zero
        after = tiles[at + 1] if at + 1 < len(tiles) else zero
        low = jnp.where(column != 0, pltpu.roll(tile, 1, 1), 0.0)
        high = jnp.where(column != NY - 1, pltpu.roll(tile, LANES - 1, 1), 0.0)
        left = pltpu.roll(jnp.where(lane < LANES - NY, tile, before), NY, 1)
        right = pltpu.roll(jnp.where(lane >= NY, tile, after), LANES - NY, 1)
        out.append((low + high) + (left + right))
    return jnp.concatenate(out, axis=1)


def lane_fold(value):
    tiles = tiles_of(value)
    while len(tiles) > 1:
        tiles = [sum(tiles[at : at + 2]) for at in range(0, len(tiles), 2)]
    return tiles[0]


def split(value):
    high = value.astype(jnp.bfloat16)
    return high, (value - high.astype(jnp.float32)).astype(jnp.bfloat16)


def kernel(
    count, doms, sliced, total_cells,
    samples, pot, gath, fin,
    sext, pot_near, pe, inv, wd, ua, ub, p1, gram, coef, mext, rhs, red,
    local_sem, halo_send, halo_recv, gram_send, gram_recv, edge_send, edge_recv,
    gath_send, gath_recv, red_send, red_recv, fin_send, fin_recv,
):
    me = lax.axis_index("shift")
    dom = lax.axis_index("dom")
    planes = pot.shape[0]
    cols, cells = sext.shape[1:]
    reps = cells // LANES
    below, above = dom > 0, dom < doms - 1

    barrier = pltpu.get_barrier_semaphore()
    for step in range(1, count):
        pl.semaphore_signal(barrier, inc=1, device_id={"shift": lax.rem(me + step, count)}, device_id_type=MESH)
    for step in range(1, doms):
        pl.semaphore_signal(barrier, inc=1, device_id={"dom": lax.rem(dom + step, doms)}, device_id_type=MESH)

    mine = pl.ds(pl.multiple_of(me * cols, 8), cols) if sliced else pl.ds(0, cols)
    own = pltpu.make_async_copy(samples.at[:, mine, :], sext.at[pl.ds(2, planes)], local_sem)
    own.start()
    pl.semaphore_wait(barrier, count - 1 + doms - 1)

    def halo(first, slot, to, to_slot):
        return (
            pltpu.make_async_remote_copy(
                samples.at[pl.ds(first, 2), mine, :], sext.at[pl.ds(slot, 2)],
                halo_send.at[to_slot, 0], halo_recv.at[to_slot, 0], {"dom": to}, device_id_type=MESH),
            pltpu.make_async_remote_copy(
                pot, pot_near.at[to_slot],
                halo_send.at[to_slot, 1], halo_recv.at[to_slot, 1], {"dom": to}, device_id_type=MESH),
        )

    up = halo(planes - 2, 0, lax.rem(dom + 1, doms), 0)
    down = halo(0, planes + 2, lax.rem(dom + doms - 1, doms), 1)

    @pl.when(above)
    def _():
        for copy in up:
            copy.start()

    @pl.when(below)
    def _():
        for copy in down:
            copy.start()

    @pl.when(jnp.logical_not(below))
    def _():
        sext[0:2] = jnp.zeros((2, cols, cells), jnp.float32)
        pot_near[0] = jnp.zeros((planes, cells), jnp.float32)

    @pl.when(jnp.logical_not(above))
    def _():
        sext[planes + 2 : planes + 4] = jnp.zeros((2, cols, cells), jnp.float32)
        pot_near[1] = jnp.zeros((planes, cells), jnp.float32)

    @pl.when(below)
    def _():
        for copy in up:
            copy.wait_recv()
        for copy in down:
            copy.wait_send()

    @pl.when(above)
    def _():
        for copy in down:
            copy.wait_recv()
        for copy in up:
            copy.wait_send()

    own.wait()
    pe[0:2] = pot_near[0, planes - 2 : planes]
    pe[2 : planes + 2] = pot[...]
    pe[planes + 2 : planes + 4] = pot_near[1, 0:2]

    for node in range(count):
        angle = math.pi * (node + 0.5) / count
        cos, sin = RADIUS * math.cos(angle), RADIUS * math.sin(angle)
        diag = (CENTRE + cos) - (6.0 + pe[...])
        over = 1.0 / (diag * diag + sin * sin)
        inv_re, inv_im = diag * over, -sin * over
        inv[node, 0] = inv_re
        inv[node, 1] = inv_im
        wd[node, 0] = (cos / count) * inv_re - (sin / count) * inv_im
        wd[node, 1] = (cos / count) * inv_im + (sin / count) * inv_re

    width = gram.shape[2]
    lane_at = lax.broadcasted_iota(jnp.int32, (cols, width), 1)

    def row(ref, node, part, at):
        return jnp.broadcast_to(ref[node, part, pl.ds(at, 1), :], (cols, cells))

    def each_node(node, packed):
        def first(at, carry):
            ua[0, at] = sext[at] * row(inv, node, 0, at)
            ua[1, at] = sext[at] * row(inv, node, 1, at)
            return carry

        lax.fori_loop(0, planes + 4, first, 0)

        def second(at, carry):
            p_re = sext[at] + (plane_sum(ua[0, at]) + (ua[0, at - 1] + ua[0, at + 1]))
            p_im = plane_sum(ua[1, at]) + (ua[1, at - 1] + ua[1, at + 1])
            p1[node, 0, at] = p_re
            p1[node, 1, at] = p_im
            i_re, i_im = row(inv, node, 0, at), row(inv, node, 1, at)
            ub[0, at] = p_re * i_re - p_im * i_im
            ub[1, at] = p_re * i_im + p_im * i_re
            return carry

        lax.fori_loop(1, planes + 3, second, 0)

        @pl.when(jnp.logical_not(below))
        def _():
            ub[0, 1] = jnp.zeros((cols, cells), jnp.float32)
            ub[1, 1] = jnp.zeros((cols, cells), jnp.float32)

        @pl.when(jnp.logical_not(above))
        def _():
            ub[0, planes + 2] = jnp.zeros((cols, cells), jnp.float32)
            ub[1, planes + 2] = jnp.zeros((cols, cells), jnp.float32)

        def third(at, sums):
            s = sext[at]
            a_re, a_im = p1[node, 0, at], p1[node, 1, at]
            b_re = a_re + (plane_sum(ub[0, at]) + (ub[0, at - 1] + ub[0, at + 1]))
            b_im = a_im + (plane_sum(ub[1, at]) + (ub[1, at - 1] + ub[1, at + 1]))
            terms = (
                a_re * a_re + a_im * a_im, a_re * s, -a_im * s,
                a_re * b_re + a_im * b_im, a_re * b_im - a_im * b_re,
                b_re * b_re + b_im * b_im, b_re * s, -b_im * s,
            )
            return tuple(old + lane_fold(term) for old, term in zip(sums, terms))

        zero = jnp.zeros((cols, LANES), jnp.float32)
        sums = lax.fori_loop(2, planes + 2, third, (zero,) * 8)
        for at, value in enumerate(sums):
            packed = jnp.where(lane_at == node * 8 + at, jnp.sum(value, axis=1, keepdims=True), packed)
        return packed

    gram[dom] = lax.fori_loop(0, count, each_node, jnp.zeros((cols, width), jnp.float32))

    def to_all(buffer, sends, recvs, axis, place, size):
        out = [
            pltpu.make_async_remote_copy(
                buffer.at[place], buffer.at[place], sends.at[step - 1], recvs.at[step - 1],
                {axis: lax.rem(place + step, size)}, device_id_type=MESH)
            for step in range(1, size)
        ]
        for copy in out:
            copy.start()
        for copy in out:
            copy.wait()

    to_all(gram, gram_send, gram_recv, "dom", dom, doms)
    total = gram[0]
    for other in range(1, doms):
        total = total + gram[other]
    g_one, q_one_re, q_one_im, g_mix_re, g_mix_im, g_two, q_two_re, q_two_im = [
        total if at == 0 else pltpu.roll(total, width - at, 1) for at in range(8)
    ]
    ridge = RIDGE * (g_one + g_two) / 2.0
    determ = (g_one + ridge) * (g_two + ridge) - (g_mix_re * g_mix_re + g_mix_im * g_mix_im)
    coefs = (
        ((g_two + ridge) * q_one_re - (g_mix_re * q_two_re - g_mix_im * q_two_im)) / determ,
        ((g_two + ridge) * q_one_im - (g_mix_re * q_two_im + g_mix_im * q_two_re)) / determ,
        ((g_one + ridge) * q_two_re - (g_mix_re * q_one_re + g_mix_im * q_one_im)) / determ,
        ((g_one + ridge) * q_two_im - (g_mix_re * q_one_im - g_mix_im * q_one_re)) / determ,
    )
    for node in range(count):
        for at, value in enumerate(coefs):
            coef[node, at] = jnp.broadcast_to(value[:, node * 8 : node * 8 + 1], (cols, LANES))

    def wide(node, at):
        return jnp.concatenate([coef[node, at]] * reps, axis=1)

    def moment(at, carry):
        s = sext[at]

        def add(node, value):
            c1r, c1i, c2r, c2i = [wide(node, part) for part in range(4)]
            a_re, a_im = p1[node, 0, at], p1[node, 1, at]
            y_re = c1r * s + c2r * a_re - c2i * a_im
            y_im = c1i * s + c2r * a_im + c2i * a_re
            return value + (row(wd, node, 0, at) * y_re - row(wd, node, 1, at) * y_im)

        value = lax.fori_loop(0, count, add, jnp.zeros((cols, cells), jnp.float32), unroll=2)
        mext[at - 1] = value
        gath[me, at - 2] = value
        rhs[at - 2, cols:] = value
        return carry

    lax.fori_loop(2, planes + 2, moment, 0)

    bits = [1 << at for at in range(count.bit_length() - 1)]
    orders = [bits[1:] + bits[:1], bits[1:][::-1] + bits[:1]]
    half = planes // 2

    def last_of(gap, order):
        return max([at for at, bit in enumerate(order) if gap & bit], default=-1)

    def hop(gap, part, at):
        bit = orders[part][at]
        where = lax.bitwise_xor(me, gap)
        block = gath.at[where, pl.ds(part * half, half if part == 0 else planes - half)]
        return pltpu.make_async_remote_copy(
            block, block, gath_send.at[part, gap, at], gath_recv.at[part, gap | bit],
            {"shift": lax.bitwise_xor(me, bit)}, device_id_type=MESH)

    def forward(gap, part, only=None):
        for at in range(last_of(gap, orders[part]) + 1, len(bits)):
            hop(gap, part, at).start()

    def arrived(gap, part):
        at = last_of(gap, orders[part])
        before = gap & ~orders[part][at]
        bit = orders[part][at]
        where = lax.bitwise_xor(me, gap)
        block = gath.at[where, pl.ds(part * half, half if part == 0 else planes - half)]
        pltpu.make_async_remote_copy(
            block, block, gath_send.at[part, before, at], gath_recv.at[part, gap],
            {"shift": lax.bitwise_xor(me, bit)}, device_id_type=MESH).wait_recv()

    def edge(plane, slot, to, to_slot):
        return pltpu.make_async_remote_copy(
            mext.at[plane], mext.at[slot], edge_send.at[to_slot], edge_recv.at[to_slot],
            {"dom": to}, device_id_type=MESH)

    edge_up = edge(planes, 0, lax.rem(dom + 1, doms), 0)
    edge_down = edge(1, planes + 1, lax.rem(dom + doms - 1, doms), 1)

    @pl.when(above)
    def _():
        edge_up.start()

    @pl.when(below)
    def _():
        edge_down.start()

    for part in range(2):
        forward(0, part)

    @pl.when(jnp.logical_not(below))
    def _():
        mext[0] = jnp.zeros((cols, cells), jnp.float32)

    @pl.when(jnp.logical_not(above))
    def _():
        mext[planes + 1] = jnp.zeros((cols, cells), jnp.float32)

    @pl.when(below)
    def _():
        edge_up.wait_recv()
        edge_down.wait_send()

    @pl.when(above)
    def _():
        edge_down.wait_recv()
        edge_up.wait_send()

    def apply(at, carry):
        onsite = 6.0 + jnp.broadcast_to(pe[pl.ds(at + 1, 1), :], (cols, cells))
        value = mext[at]
        rhs[at - 1, :cols] = onsite * value - (plane_sum(value) + (mext[at - 1] + mext[at + 1]))
        return carry

    lax.fori_loop(1, planes + 1, apply, 0)

    arrivals = sorted(
        ((gap, part) for gap in range(1, count) for part in range(2)),
        key=lambda pair: (pair[0] & 1, bin(pair[0]).count("1"), last_of(pair[0], orders[pair[1]]), pair[1]))
    for gap, part in arrivals:
        arrived(gap, part)
        forward(gap, part)

    def contract(at, value):
        left_hi, left_lo = split(rhs[at])
        right_hi, right_lo = split(gath[:, at].reshape(count * cols, cells))
        dims = (((1,), (1,)), ((), ()))
        dot = functools.partial(lax.dot_general, dimension_numbers=dims, preferred_element_type=jnp.float32)
        return value + (dot(left_hi, right_hi) + (dot(left_hi, right_lo) + dot(left_lo, right_hi)))

    value = lax.fori_loop(0, planes, contract, jnp.zeros((2 * cols, count * cols), jnp.float32))
    red[dom] = value
    to_all(red, red_send, red_recv, "dom", dom, doms)
    total = red[0]
    for other in range(1, doms):
        total = total + red[other]
    fin[me] = total * (1.0 / total_cells)
    to_all(fin, fin_send, fin_recv, "shift", me, count)

    for part in range(2):
        for gap in range(count):
            for at in range(last_of(gap, orders[part]) + 1, len(bits)):
                hop(gap, part, at).wait_send()


def on_device(count, doms, samples, potential):
    planes, vectors, cells = samples.shape
    own = vectors // count
    cols = -(-own // 8) * 8
    sliced = own == cols
    if not sliced:
        part = lax.dynamic_slice_in_dim(samples, lax.axis_index("shift") * own, own, axis=1)
        samples = jnp.pad(part, ((0, 0), (0, cols - own), (0, 0)))
    width = -(-count * 8 // LANES) * LANES
    levels = count.bit_length() - 1
    f32 = jnp.float32
    dma = pltpu.SemaphoreType.DMA
    vmem = pl.BlockSpec(memory_space=pltpu.VMEM)
    gath, fin = pl.pallas_call(
        functools.partial(kernel, count, doms, sliced, planes * doms * cells),
        out_shape=(
            jax.ShapeDtypeStruct((count, planes, cols, cells), f32),
            jax.ShapeDtypeStruct((count, 2 * cols, count * cols), f32),
        ),
        in_specs=[pl.BlockSpec(memory_space=pl.ANY), vmem],
        out_specs=(vmem, vmem),
        scratch_shapes=[
            pltpu.VMEM((planes + 4, cols, cells), f32),
            pltpu.VMEM((2, planes, cells), f32),
            pltpu.VMEM((planes + 4, cells), f32),
            pltpu.VMEM((count, 2, planes + 4, cells), f32),
            pltpu.VMEM((count, 2, planes + 4, cells), f32),
            pltpu.VMEM((2, planes + 4, cols, cells), f32),
            pltpu.VMEM((2, planes + 4, cols, cells), f32),
            pltpu.VMEM((count, 2, planes + 4, cols, cells), f32),
            pltpu.VMEM((doms, cols, width), f32),
            pltpu.VMEM((count, 4, cols, LANES), f32),
            pltpu.VMEM((planes + 2, cols, cells), f32),
            pltpu.VMEM((planes, 2 * cols, cells), f32),
            pltpu.VMEM((doms, 2 * cols, count * cols), f32),
            dma,
            dma((2, 2)), dma((2, 2)),
            dma((doms,)), dma((doms,)),
            dma((2,)), dma((2,)),
            dma((2, count, levels)), dma((2, count)),
            dma((doms,)), dma((doms,)),
            dma((count,)), dma((count,)),
        ],
        compiler_params=pltpu.CompilerParams(
            collective_id=0, has_side_effects=True, vmem_limit_bytes=56 * 1024 * 1024
        ),
        name="feast_step",
    )(samples, potential)
    subspace = jnp.transpose(gath[:, :, :own], (1, 0, 2, 3)).reshape(planes, vectors, cells)
    fin = fin.reshape(count, 2, cols, count, cols)[:, :, :own, :, :own]
    fin = jnp.transpose(fin, (1, 3, 4, 0, 2)).reshape(2, vectors, vectors)
    return subspace, fin[0], fin[1]


def solution(mesh):
    in_specs = (P("dom", None, None), P("dom", None))
    out_specs = (P("dom", None, None), P(), P())
    return jax.shard_map(
        functools.partial(on_device, mesh.shape["shift"], mesh.shape["dom"]),
        mesh=mesh, in_specs=in_specs, out_specs=out_specs, check_vma=False,
    )
```

```python
import functools
import math

import jax
import jax.numpy as jnp
from jax import lax
from jax.experimental import pallas as pl
from jax.experimental.pallas import tpu as pltpu
from jax.sharding import PartitionSpec as P

NX = 32
NY = 32
LANES = 128

CENTRE = 3.0
RADIUS = 2.0
RIDGE = 0.01
MESH = pl.DeviceIdType.MESH


def tiles_of(value):
    return [value[:, at : at + LANES] for at in range(0, value.shape[1], LANES)]


def lane_of(value):
    return lax.broadcasted_iota(jnp.int32, value.shape, 1)


def spread(tiles):
    count, per = len(tiles), LANES // NY
    block = lane_of(tiles[0]) // NY
    out = []
    for at in range(count):
        for to in range(per):
            x = to * count + at
            part = tiles[x // per]
            move = (NY * (to - x % per)) % LANES
            part = pltpu.roll(part, move, 1) if move else part
            value = part if to == 0 else jnp.where(block == to, part, value)
        out.append(value)
    return out


def gather_back(tiles):
    count, per = len(tiles), LANES // NY
    block = lane_of(tiles[0]) // NY
    out = []
    for at in range(count):
        for to in range(per):
            x = at * per + to
            part = tiles[x % count]
            move = (NY * (to - x // count)) % LANES
            part = pltpu.roll(part, move, 1) if move else part
            value = part if to == 0 else jnp.where(block == to, part, value)
        out.append(value)
    return out


def neighbours(get, at, tile, count):
    here = get(at, tile)
    lane = lane_of(here)
    column = lane % NY
    low = jnp.where(column != 0, pltpu.roll(here, 1, 1), 0.0)
    high = jnp.where(column != NY - 1, pltpu.roll(here, LANES - 1, 1), 0.0)
    if tile > 0:
        left = get(at, tile - 1)
    else:
        left = jnp.where(lane >= NY, pltpu.roll(get(at, count - 1), NY, 1), 0.0)
    if tile < count - 1:
        right = get(at, tile + 1)
    else:
        right = jnp.where(lane < LANES - NY, pltpu.roll(get(at, 0), LANES - NY, 1), 0.0)
    return ((low + high) + (left + right)) + (get(at - 1, tile) + get(at + 1, tile))


def split(value):
    high = value.astype(jnp.bfloat16)
    return high, (value - high.astype(jnp.float32)).astype(jnp.bfloat16)


def kernel(
    count, doms, sliced, total_cells,
    samples, pot, gath, fin,
    sraw, sext, pot_near, pe, inv, wd, ua, ub, p1, gram, coef, mext, rhs, red,
    local_sem, halo_send, halo_recv, gram_send, gram_recv, edge_send, edge_recv,
    gath_send, gath_recv, red_send, red_recv, fin_send, fin_recv,
):
    me = lax.axis_index("shift")
    dom = lax.axis_index("dom")
    planes = pot.shape[0]
    cols, cells = sext.shape[1:]
    reps = cells // LANES
    below, above = dom > 0, dom < doms - 1

    def lanes(tile):
        return pl.ds(tile * LANES, LANES)


    barrier = pltpu.get_barrier_semaphore()
    for step in range(1, count):
        pl.semaphore_signal(barrier, inc=1, device_id={"shift": lax.rem(me + step, count)}, device_id_type=MESH)
    for step in range(1, doms):
        pl.semaphore_signal(barrier, inc=1, device_id={"dom": lax.rem(dom + step, doms)}, device_id_type=MESH)

    mine = pl.ds(pl.multiple_of(me * cols, 8), cols) if sliced else pl.ds(0, cols)
    own = pltpu.make_async_copy(samples.at[:, mine, :], sraw.at[pl.ds(2, planes)], local_sem)
    own.start()
    pl.semaphore_wait(barrier, count - 1 + doms - 1)

    def halo(first, slot, to, to_slot):
        return (
            pltpu.make_async_remote_copy(
                samples.at[pl.ds(first, 2), mine, :], sraw.at[pl.ds(slot, 2)],
                halo_send.at[to_slot, 0], halo_recv.at[to_slot, 0], {"dom": to}, device_id_type=MESH),
            pltpu.make_async_remote_copy(
                pot, pot_near.at[to_slot],
                halo_send.at[to_slot, 1], halo_recv.at[to_slot, 1], {"dom": to}, device_id_type=MESH),
        )

    up = halo(planes - 2, 0, lax.rem(dom + 1, doms), 0)
    down = halo(0, planes + 2, lax.rem(dom + doms - 1, doms), 1)

    @pl.when(above)
    def _():
        for copy in up:
            copy.start()

    @pl.when(below)
    def _():
        for copy in down:
            copy.start()

    @pl.when(jnp.logical_not(below))
    def _():
        sraw[0:2] = jnp.zeros((2, cols, cells), jnp.float32)
        pot_near[0] = jnp.zeros((planes, cells), jnp.float32)

    @pl.when(jnp.logical_not(above))
    def _():
        sraw[planes + 2 : planes + 4] = jnp.zeros((2, cols, cells), jnp.float32)
        pot_near[1] = jnp.zeros((planes, cells), jnp.float32)

    @pl.when(below)
    def _():
        for copy in up:
            copy.wait_recv()
        for copy in down:
            copy.wait_send()

    @pl.when(above)
    def _():
        for copy in down:
            copy.wait_recv()
        for copy in up:
            copy.wait_send()

    own.wait()
    pe[0:2] = pot_near[0, planes - 2 : planes]
    pe[2 : planes + 2] = pot[...]
    pe[planes + 2 : planes + 4] = pot_near[1, 0:2]

    for at, tile in enumerate(spread(tiles_of(pe[...]))):
        pe[:, lanes(at)] = tile

    def spread_plane(at, carry):
        for tile, value in enumerate(spread(tiles_of(sraw[at]))):
            sext[at, :, lanes(tile)] = value
        return carry

    lax.fori_loop(0, planes + 4, spread_plane, 0)

    for node in range(count):
        angle = math.pi * (node + 0.5) / count
        cos, sin = RADIUS * math.cos(angle), RADIUS * math.sin(angle)
        diag = (CENTRE + cos) - (6.0 + pe[...])
        over = 1.0 / (diag * diag + sin * sin)
        inv_re, inv_im = diag * over, -sin * over
        inv[node, 0] = inv_re
        inv[node, 1] = inv_im
        wd[node, 0] = (cos / count) * inv_re - (sin / count) * inv_im
        wd[node, 1] = (cos / count) * inv_im + (sin / count) * inv_re

    width = gram.shape[2]
    lane_at = lax.broadcasted_iota(jnp.int32, (cols, width), 1)

    def row(ref, node, part, at, tile):
        return jnp.broadcast_to(ref[node, part, at : at + 1, lanes(tile)], (cols, LANES))

    def field(ref, part, centre):
        seen = {}

        def get(shift, tile):
            if (shift, tile) not in seen:
                seen[shift, tile] = ref[part, centre + shift, :, lanes(tile)]
            return seen[shift, tile]

        return get

    def each_node(node, packed):
        def first(at):
            for tile in range(reps):
                s = sext[at, :, lanes(tile)]
                ua[0, at, :, lanes(tile)] = s * row(inv, node, 0, at, tile)
                ua[1, at, :, lanes(tile)] = s * row(inv, node, 1, at, tile)

        for at in range(0, planes + 4):
            first(at)

        def second(at):
            u_re, u_im = field(ua, 0, at), field(ua, 1, at)
            for tile in range(reps):
                p_re = sext[at, :, lanes(tile)] + neighbours(u_re, 0, tile, reps)
                p_im = neighbours(u_im, 0, tile, reps)
                p1[node, 0, at, :, lanes(tile)] = p_re
                p1[node, 1, at, :, lanes(tile)] = p_im
                i_re, i_im = row(inv, node, 0, at, tile), row(inv, node, 1, at, tile)
                ub[0, at, :, lanes(tile)] = p_re * i_re - p_im * i_im
                ub[1, at, :, lanes(tile)] = p_re * i_im + p_im * i_re

        for at in range(1, planes + 3):
            second(at)

        @pl.when(jnp.logical_not(below))
        def _():
            ub[0, 1] = jnp.zeros((cols, cells), jnp.float32)
            ub[1, 1] = jnp.zeros((cols, cells), jnp.float32)

        @pl.when(jnp.logical_not(above))
        def _():
            ub[0, planes + 2] = jnp.zeros((cols, cells), jnp.float32)
            ub[1, planes + 2] = jnp.zeros((cols, cells), jnp.float32)

        def third(at, sums):
            u_re, u_im = field(ub, 0, at), field(ub, 1, at)
            for tile in range(reps):
                s = sext[at, :, lanes(tile)]
                a_re, a_im = p1[node, 0, at, :, lanes(tile)], p1[node, 1, at, :, lanes(tile)]
                b_re = a_re + neighbours(u_re, 0, tile, reps)
                b_im = a_im + neighbours(u_im, 0, tile, reps)
                terms = (
                    a_re * a_re + a_im * a_im, a_re * s, -(a_im * s),
                    a_re * b_re + a_im * b_im, a_re * b_im - a_im * b_re,
                    b_re * b_re + b_im * b_im, b_re * s, -(b_im * s),
                )
                sums = tuple(old + term for old, term in zip(sums, terms))
            return sums

        zero = jnp.zeros((cols, LANES), jnp.float32)
        sums = lax.fori_loop(2, planes + 2, third, (zero,) * 8)
        for at, value in enumerate(sums):
            packed = jnp.where(lane_at == node * 8 + at, jnp.sum(value, axis=1, keepdims=True), packed)
        return packed

    gram[dom] = lax.fori_loop(0, count, each_node, jnp.zeros((cols, width), jnp.float32))

    def to_all(buffer, sends, recvs, axis, place, size):
        out = [
            pltpu.make_async_remote_copy(
                buffer.at[place], buffer.at[place], sends.at[step - 1], recvs.at[step - 1],
                {axis: lax.rem(place + step, size)}, device_id_type=MESH)
            for step in range(1, size)
        ]
        for copy in out:
            copy.start()
        for copy in out:
            copy.wait()

    to_all(gram, gram_send, gram_recv, "dom", dom, doms)
    total = gram[0]
    for other in range(1, doms):
        total = total + gram[other]
    g_one, q_one_re, q_one_im, g_mix_re, g_mix_im, g_two, q_two_re, q_two_im = [
        total if at == 0 else pltpu.roll(total, width - at, 1) for at in range(8)
    ]
    ridge = RIDGE * (g_one + g_two) / 2.0
    determ = (g_one + ridge) * (g_two + ridge) - (g_mix_re * g_mix_re + g_mix_im * g_mix_im)
    coefs = (
        ((g_two + ridge) * q_one_re - (g_mix_re * q_two_re - g_mix_im * q_two_im)) / determ,
        ((g_two + ridge) * q_one_im - (g_mix_re * q_two_im + g_mix_im * q_two_re)) / determ,
        ((g_one + ridge) * q_two_re - (g_mix_re * q_one_re + g_mix_im * q_one_im)) / determ,
        ((g_one + ridge) * q_two_im - (g_mix_re * q_one_im - g_mix_im * q_one_re)) / determ,
    )
    for node in range(count):
        for at, value in enumerate(coefs):
            coef[node, at] = jnp.broadcast_to(value[:, node * 8 : node * 8 + 1], (cols, LANES))

    def moment(at):
        values = [jnp.zeros((cols, LANES), jnp.float32)] * reps
        for node in range(count):
            c1r, c1i, c2r, c2i = [coef[node, part] for part in range(4)]
            for tile in range(reps):
                s = sext[at, :, lanes(tile)]
                a_re, a_im = p1[node, 0, at, :, lanes(tile)], p1[node, 1, at, :, lanes(tile)]
                y_re = c1r * s + (c2r * a_re - c2i * a_im)
                y_im = c1i * s + (c2r * a_im + c2i * a_re)
                values[tile] = values[tile] + (
                    row(wd, node, 0, at, tile) * y_re - row(wd, node, 1, at, tile) * y_im)
        for tile, value in enumerate(values):
            mext[0, at - 1, :, lanes(tile)] = value
        for tile, value in enumerate(gather_back(values)):
            gath[me, at - 2, :, lanes(tile)] = value
            rhs[at - 2, cols:, lanes(tile)] = value

    for at in range(2, planes + 2):
        moment(at)

    bits = [1 << at for at in range(count.bit_length() - 1)]
    orders = [bits[1:] + bits[:1], bits[1:][::-1] + bits[:1]]
    half = planes // 2

    def last_of(gap, order):
        return max([at for at, bit in enumerate(order) if gap & bit], default=-1)

    def hop(gap, part, at):
        bit = orders[part][at]
        where = lax.bitwise_xor(me, gap)
        block = gath.at[where, pl.ds(part * half, half if part == 0 else planes - half)]
        return pltpu.make_async_remote_copy(
            block, block, gath_send.at[part, gap, at], gath_recv.at[part, gap | bit],
            {"shift": lax.bitwise_xor(me, bit)}, device_id_type=MESH)

    def forward(gap, part, only=None):
        for at in range(last_of(gap, orders[part]) + 1, len(bits)):
            hop(gap, part, at).start()

    def arrived(gap, part):
        at = last_of(gap, orders[part])
        before = gap & ~orders[part][at]
        bit = orders[part][at]
        where = lax.bitwise_xor(me, gap)
        block = gath.at[where, pl.ds(part * half, half if part == 0 else planes - half)]
        pltpu.make_async_remote_copy(
            block, block, gath_send.at[part, before, at], gath_recv.at[part, gap],
            {"shift": lax.bitwise_xor(me, bit)}, device_id_type=MESH).wait_recv()

    def edge(plane, slot, to, to_slot):
        return pltpu.make_async_remote_copy(
            mext.at[0, plane], mext.at[0, slot], edge_send.at[to_slot], edge_recv.at[to_slot],
            {"dom": to}, device_id_type=MESH)

    edge_up = edge(planes, 0, lax.rem(dom + 1, doms), 0)
    edge_down = edge(1, planes + 1, lax.rem(dom + doms - 1, doms), 1)

    @pl.when(above)
    def _():
        edge_up.start()

    @pl.when(below)
    def _():
        edge_down.start()

    for part in range(2):
        forward(0, part)

    @pl.when(jnp.logical_not(below))
    def _():
        mext[0, 0] = jnp.zeros((cols, cells), jnp.float32)

    @pl.when(jnp.logical_not(above))
    def _():
        mext[0, planes + 1] = jnp.zeros((cols, cells), jnp.float32)

    @pl.when(below)
    def _():
        edge_up.wait_recv()
        edge_down.wait_send()

    @pl.when(above)
    def _():
        edge_down.wait_recv()
        edge_up.wait_send()

    def apply(at):
        get = field(mext, 0, at)
        values = []
        for tile in range(reps):
            onsite = 6.0 + jnp.broadcast_to(pe[at + 1 : at + 2, lanes(tile)], (cols, LANES))
            values.append(onsite * get(0, tile) - neighbours(get, 0, tile, reps))
        for tile, value in enumerate(gather_back(values)):
            rhs[at - 1, :cols, lanes(tile)] = value

    for at in range(1, planes + 1):
        apply(at)

    arrivals = sorted(
        ((gap, part) for gap in range(1, count) for part in range(2)),
        key=lambda pair: (pair[0] & 1, bin(pair[0]).count("1"), last_of(pair[0], orders[pair[1]]), pair[1]))
    for gap, part in arrivals:
        arrived(gap, part)
        forward(gap, part)

    def contract(at, value):
        left_hi, left_lo = split(rhs[at])
        right_hi, right_lo = split(gath[:, at].reshape(count * cols, cells))
        dims = (((1,), (1,)), ((), ()))
        dot = functools.partial(lax.dot_general, dimension_numbers=dims, preferred_element_type=jnp.float32)
        return value + (dot(left_hi, right_hi) + (dot(left_hi, right_lo) + dot(left_lo, right_hi)))

    value = lax.fori_loop(0, planes, contract, jnp.zeros((2 * cols, count * cols), jnp.float32))
    red[dom] = value
    to_all(red, red_send, red_recv, "dom", dom, doms)
    total = red[0]
    for other in range(1, doms):
        total = total + red[other]
    fin[me] = total * (1.0 / total_cells)
    to_all(fin, fin_send, fin_recv, "shift", me, count)

    for part in range(2):
        for gap in range(count):
            for at in range(last_of(gap, orders[part]) + 1, len(bits)):
                hop(gap, part, at).wait_send()


def on_device(count, doms, samples, potential):
    planes, vectors, cells = samples.shape
    own = vectors // count
    cols = -(-own // 8) * 8
    sliced = own == cols
    if not sliced:
        part = lax.dynamic_slice_in_dim(samples, lax.axis_index("shift") * own, own, axis=1)
        samples = jnp.pad(part, ((0, 0), (0, cols - own), (0, 0)))
    width = -(-count * 8 // LANES) * LANES
    levels = count.bit_length() - 1
    f32 = jnp.float32
    dma = pltpu.SemaphoreType.DMA
    vmem = pl.BlockSpec(memory_space=pltpu.VMEM)
    gath, fin = pl.pallas_call(
        functools.partial(kernel, count, doms, sliced, planes * doms * cells),
        out_shape=(
            jax.ShapeDtypeStruct((count, planes, cols, cells), f32),
            jax.ShapeDtypeStruct((count, 2 * cols, count * cols), f32),
        ),
        in_specs=[pl.BlockSpec(memory_space=pl.ANY), vmem],
        out_specs=(vmem, vmem),
        scratch_shapes=[
            pltpu.VMEM((planes + 4, cols, cells), f32),
            pltpu.VMEM((planes + 4, cols, cells), f32),
            pltpu.VMEM((2, planes, cells), f32),
            pltpu.VMEM((planes + 4, cells), f32),
            pltpu.VMEM((count, 2, planes + 4, cells), f32),
            pltpu.VMEM((count, 2, planes + 4, cells), f32),
            pltpu.VMEM((2, planes + 4, cols, cells), f32),
            pltpu.VMEM((2, planes + 4, cols, cells), f32),
            pltpu.VMEM((count, 2, planes + 4, cols, cells), f32),
            pltpu.VMEM((doms, cols, width), f32),
            pltpu.VMEM((count, 4, cols, LANES), f32),
            pltpu.VMEM((1, planes + 2, cols, cells), f32),
            pltpu.VMEM((planes, 2 * cols, cells), f32),
            pltpu.VMEM((doms, 2 * cols, count * cols), f32),
            dma,
            dma((2, 2)), dma((2, 2)),
            dma((doms,)), dma((doms,)),
            dma((2,)), dma((2,)),
            dma((2, count, levels)), dma((2, count)),
            dma((doms,)), dma((doms,)),
            dma((count,)), dma((count,)),
        ],
        compiler_params=pltpu.CompilerParams(
            collective_id=0, has_side_effects=True, vmem_limit_bytes=56 * 1024 * 1024
        ),
        name="feast_step",
    )(samples, potential)
    subspace = jnp.transpose(gath[:, :, :own], (1, 0, 2, 3)).reshape(planes, vectors, cells)
    fin = fin.reshape(count, 2, cols, count, cols)[:, :, :own, :, :own]
    fin = jnp.transpose(fin, (1, 3, 4, 0, 2)).reshape(2, vectors, vectors)
    return subspace, fin[0], fin[1]


def solution(mesh):
    in_specs = (P("dom", None, None), P("dom", None))
    out_specs = (P("dom", None, None), P(), P())
    return jax.shard_map(
        functools.partial(on_device, mesh.shape["shift"], mesh.shape["dom"]),
        mesh=mesh, in_specs=in_specs, out_specs=out_specs, check_vma=False,
    )
```

```python
import functools
import math

import jax
import jax.numpy as jnp
from jax import lax
from jax.experimental import pallas as pl
from jax.experimental.pallas import tpu as pltpu
from jax.sharding import PartitionSpec as P

NX = 32
NY = 32
LANES = 128

CENTRE = 3.0
RADIUS = 2.0
RIDGE = 0.01
MESH = pl.DeviceIdType.MESH


def tiles_of(value):
    return [value[:, at : at + LANES] for at in range(0, value.shape[1], LANES)]


def lane_of(value):
    return lax.broadcasted_iota(jnp.int32, value.shape, 1)


def spread(tiles):
    count, per = len(tiles), LANES // NY
    block = lane_of(tiles[0]) // NY
    out = []
    for at in range(count):
        for to in range(per):
            x = to * count + at
            part = tiles[x // per]
            move = (NY * (to - x % per)) % LANES
            part = pltpu.roll(part, move, 1) if move else part
            value = part if to == 0 else jnp.where(block == to, part, value)
        out.append(value)
    return out


def gather_back(tiles):
    count, per = len(tiles), LANES // NY
    block = lane_of(tiles[0]) // NY
    out = []
    for at in range(count):
        for to in range(per):
            x = at * per + to
            part = tiles[x % count]
            move = (NY * (to - x // count)) % LANES
            part = pltpu.roll(part, move, 1) if move else part
            value = part if to == 0 else jnp.where(block == to, part, value)
        out.append(value)
    return out


def neighbours(get, at, tile, count):
    here = get(at, tile)
    lane = lane_of(here)
    column = lane % NY
    low = jnp.where(column != 0, pltpu.roll(here, 1, 1), 0.0)
    high = jnp.where(column != NY - 1, pltpu.roll(here, LANES - 1, 1), 0.0)
    if tile > 0:
        left = get(at, tile - 1)
    else:
        left = jnp.where(lane >= NY, pltpu.roll(get(at, count - 1), NY, 1), 0.0)
    if tile < count - 1:
        right = get(at, tile + 1)
    else:
        right = jnp.where(lane < LANES - NY, pltpu.roll(get(at, 0), LANES - NY, 1), 0.0)
    return ((low + high) + (left + right)) + (get(at - 1, tile) + get(at + 1, tile))


def split(value):
    high = value.astype(jnp.bfloat16)
    return high, (value - high.astype(jnp.float32)).astype(jnp.bfloat16)


def kernel(
    count, doms, sliced, total_cells,
    samples, pot, out, out_h, out_b,
    gath, fin,
    sraw, sext, pot_near, pe, inv, wd, ua, ub, p1, gram, coef, mext, rhs, red,
    local_sem, halo_send, halo_recv, gram_send, gram_recv, edge_send, edge_recv,
    gath_send, gath_recv, out_sem, red_send, red_recv, fin_send, fin_recv,
):
    me = lax.axis_index("shift")
    dom = lax.axis_index("dom")
    planes = pot.shape[0]
    cols, cells = sext.shape[1:]
    reps = cells // LANES
    below, above = dom > 0, dom < doms - 1

    def lanes(tile):
        return pl.ds(tile * LANES, LANES)


    barrier = pltpu.get_barrier_semaphore()
    for step in range(1, count):
        pl.semaphore_signal(barrier, inc=1, device_id={"shift": lax.rem(me + step, count)}, device_id_type=MESH)
    for step in range(1, doms):
        pl.semaphore_signal(barrier, inc=1, device_id={"dom": lax.rem(dom + step, doms)}, device_id_type=MESH)

    mine = pl.ds(pl.multiple_of(me * cols, 8), cols) if sliced else pl.ds(0, cols)
    own = pltpu.make_async_copy(samples.at[:, mine, :], sraw.at[pl.ds(2, planes)], local_sem)
    own.start()
    pl.semaphore_wait(barrier, count - 1 + doms - 1)

    def halo(first, slot, to, to_slot):
        return (
            pltpu.make_async_remote_copy(
                samples.at[pl.ds(first, 2), mine, :], sraw.at[pl.ds(slot, 2)],
                halo_send.at[to_slot, 0], halo_recv.at[to_slot, 0], {"dom": to}, device_id_type=MESH),
            pltpu.make_async_remote_copy(
                pot, pot_near.at[to_slot],
                halo_send.at[to_slot, 1], halo_recv.at[to_slot, 1], {"dom": to}, device_id_type=MESH),
        )

    up = halo(planes - 2, 0, lax.rem(dom + 1, doms), 0)
    down = halo(0, planes + 2, lax.rem(dom + doms - 1, doms), 1)

    @pl.when(above)
    def _():
        for copy in up:
            copy.start()

    @pl.when(below)
    def _():
        for copy in down:
            copy.start()

    @pl.when(jnp.logical_not(below))
    def _():
        sraw[0:2] = jnp.zeros((2, cols, cells), jnp.float32)
        pot_near[0] = jnp.zeros((planes, cells), jnp.float32)

    @pl.when(jnp.logical_not(above))
    def _():
        sraw[planes + 2 : planes + 4] = jnp.zeros((2, cols, cells), jnp.float32)
        pot_near[1] = jnp.zeros((planes, cells), jnp.float32)

    def row_at(at):
        if at < 2:
            return planes + at
        return at - 2 if at < planes + 2 else at

    def diagonals(rows):
        for tile, value in enumerate(spread(tiles_of(pe[rows]))):
            pe[rows, lanes(tile)] = value
        for node in range(count):
            angle = math.pi * (node + 0.5) / count
            cos, sin = RADIUS * math.cos(angle), RADIUS * math.sin(angle)
            diag = (CENTRE + cos) - (6.0 + pe[rows])
            over = 1.0 / (diag * diag + sin * sin)
            inv_re, inv_im = diag * over, -sin * over
            inv[node, 0, rows] = inv_re
            inv[node, 1, rows] = inv_im
            wd[node, 0, rows] = (cos / count) * inv_re - (sin / count) * inv_im
            wd[node, 1, rows] = (cos / count) * inv_im + (sin / count) * inv_re

    def spread_plane(at, carry):
        for tile, value in enumerate(spread(tiles_of(sraw[at]))):
            sext[at, :, lanes(tile)] = value
        return carry

    pe[0:planes] = pot[...]
    diagonals(slice(0, planes))
    own.wait()
    lax.fori_loop(2, planes + 2, spread_plane, 0)

    width = gram.shape[2]
    lane_at = lax.broadcasted_iota(jnp.int32, (cols, width), 1)

    def row(ref, node, part, at, tile):
        return jnp.broadcast_to(ref[node, part, row_at(at) : row_at(at) + 1, lanes(tile)], (cols, LANES))

    def field(ref, part, centre):
        seen = {}

        def get(shift, tile):
            if (shift, tile) not in seen:
                seen[shift, tile] = ref[part, centre + shift, :, lanes(tile)]
            return seen[shift, tile]

        return get

    edge_planes = (1, 2, planes + 1, planes + 2)

    def inner(node, carry):
        one_node(node, range(2, planes + 2), range(3, planes + 1))
        return carry

    def one_node(node, firsts, seconds):
        def first(at):
            for tile in range(reps):
                s = sext[at, :, lanes(tile)]
                ua[node, 0, at, :, lanes(tile)] = s * row(inv, node, 0, at, tile)
                ua[node, 1, at, :, lanes(tile)] = s * row(inv, node, 1, at, tile)


        def second(at):
            u_re, u_im = field(ua.at[node], 0, at), field(ua.at[node], 1, at)
            for tile in range(reps):
                p_re = sext[at, :, lanes(tile)] + neighbours(u_re, 0, tile, reps)
                p_im = neighbours(u_im, 0, tile, reps)
                p1[node, 0, at, :, lanes(tile)] = p_re
                p1[node, 1, at, :, lanes(tile)] = p_im
                i_re, i_im = row(inv, node, 0, at, tile), row(inv, node, 1, at, tile)
                ub[node, 0, at, :, lanes(tile)] = p_re * i_re - p_im * i_im
                ub[node, 1, at, :, lanes(tile)] = p_re * i_im + p_im * i_re

        for at in firsts:
            first(at)
        for at in seconds:
            second(at)

    lax.fori_loop(0, count, inner, 0)

    @pl.when(below)
    def _():
        for copy in up:
            copy.wait_recv()
        for copy in down:
            copy.wait_send()

    @pl.when(above)
    def _():
        for copy in down:
            copy.wait_recv()
        for copy in up:
            copy.wait_send()

    pe[planes : planes + 2] = pot_near[0, planes - 2 : planes]
    pe[planes + 2 : planes + 4] = pot_near[1, 0:2]
    diagonals(slice(planes, planes + 4))
    for at in (0, 1, planes + 2, planes + 3):
        spread_plane(at, 0)

    def each_node(node, packed):
        one_node(node, (0, 1, planes + 2, planes + 3), edge_planes)

        @pl.when(jnp.logical_not(below))
        def _():
            ub[node, 0, 1] = jnp.zeros((cols, cells), jnp.float32)
            ub[node, 1, 1] = jnp.zeros((cols, cells), jnp.float32)

        @pl.when(jnp.logical_not(above))
        def _():
            ub[node, 0, planes + 2] = jnp.zeros((cols, cells), jnp.float32)
            ub[node, 1, planes + 2] = jnp.zeros((cols, cells), jnp.float32)

        def third(at, sums):
            u_re, u_im = field(ub.at[node], 0, at), field(ub.at[node], 1, at)
            for tile in range(reps):
                s = sext[at, :, lanes(tile)]
                a_re, a_im = p1[node, 0, at, :, lanes(tile)], p1[node, 1, at, :, lanes(tile)]
                b_re = a_re + neighbours(u_re, 0, tile, reps)
                b_im = a_im + neighbours(u_im, 0, tile, reps)
                terms = (
                    a_re * a_re + a_im * a_im, a_re * s, -(a_im * s),
                    a_re * b_re + a_im * b_im, a_re * b_im - a_im * b_re,
                    b_re * b_re + b_im * b_im, b_re * s, -(b_im * s),
                )
                sums = tuple(old + term for old, term in zip(sums, terms))
            return sums

        zero = jnp.zeros((cols, LANES), jnp.float32)
        sums = lax.fori_loop(2, planes + 2, third, (zero,) * 8)
        for at, value in enumerate(sums):
            packed = jnp.where(lane_at == node * 8 + at, jnp.sum(value, axis=1, keepdims=True), packed)
        return packed

    gram[dom] = lax.fori_loop(0, count, each_node, jnp.zeros((cols, width), jnp.float32))

    def to_all(buffer, sends, recvs, axis, place, size):
        out = [
            pltpu.make_async_remote_copy(
                buffer.at[place], buffer.at[place], sends.at[step - 1], recvs.at[step - 1],
                {axis: lax.rem(place + step, size)}, device_id_type=MESH)
            for step in range(1, size)
        ]
        for copy in out:
            copy.start()
        for copy in out:
            copy.wait()

    to_all(gram, gram_send, gram_recv, "dom", dom, doms)
    total = gram[0]
    for other in range(1, doms):
        total = total + gram[other]
    g_one, q_one_re, q_one_im, g_mix_re, g_mix_im, g_two, q_two_re, q_two_im = [
        total if at == 0 else pltpu.roll(total, width - at, 1) for at in range(8)
    ]
    ridge = RIDGE * (g_one + g_two) / 2.0
    determ = (g_one + ridge) * (g_two + ridge) - (g_mix_re * g_mix_re + g_mix_im * g_mix_im)
    coefs = (
        ((g_two + ridge) * q_one_re - (g_mix_re * q_two_re - g_mix_im * q_two_im)) / determ,
        ((g_two + ridge) * q_one_im - (g_mix_re * q_two_im + g_mix_im * q_two_re)) / determ,
        ((g_one + ridge) * q_two_re - (g_mix_re * q_one_re + g_mix_im * q_one_im)) / determ,
        ((g_one + ridge) * q_two_im - (g_mix_re * q_one_im - g_mix_im * q_one_re)) / determ,
    )
    for node in range(count):
        for at, value in enumerate(coefs):
            coef[node, at] = jnp.broadcast_to(value[:, node * 8 : node * 8 + 1], (cols, LANES))

    def moment(at):
        values = [jnp.zeros((cols, LANES), jnp.float32)] * reps
        for node in range(count):
            c1r, c1i, c2r, c2i = [coef[node, part] for part in range(4)]
            for tile in range(reps):
                s = sext[at, :, lanes(tile)]
                a_re, a_im = p1[node, 0, at, :, lanes(tile)], p1[node, 1, at, :, lanes(tile)]
                y_re = c1r * s + (c2r * a_re - c2i * a_im)
                y_im = c1i * s + (c2r * a_im + c2i * a_re)
                values[tile] = values[tile] + (
                    row(wd, node, 0, at, tile) * y_re - row(wd, node, 1, at, tile) * y_im)
        for tile, value in enumerate(values):
            mext[0, at - 1, :, lanes(tile)] = value
        for tile, value in enumerate(gather_back(values)):
            gath[me, at - 2, :, lanes(tile)] = value
            rhs[at - 2, cols:, lanes(tile)] = value


    bits = [1 << at for at in range(count.bit_length() - 1)]
    orders = [bits[1:] + bits[:1], bits[1:][::-1] + bits[:1]]
    half = planes // 2

    def last_of(gap, order):
        return max([at for at, bit in enumerate(order) if gap & bit], default=-1)

    def hop(gap, part, at):
        bit = orders[part][at]
        where = lax.bitwise_xor(me, gap)
        block = gath.at[where, pl.ds(part * half, half if part == 0 else planes - half)]
        return pltpu.make_async_remote_copy(
            block, block, gath_send.at[part, gap, at], gath_recv.at[part, gap | bit],
            {"shift": lax.bitwise_xor(me, bit)}, device_id_type=MESH)

    def forward(gap, part, only=None):
        for at in range(last_of(gap, orders[part]) + 1, len(bits)):
            hop(gap, part, at).start()

    def arrived(gap, part):
        at = last_of(gap, orders[part])
        before = gap & ~orders[part][at]
        bit = orders[part][at]
        where = lax.bitwise_xor(me, gap)
        block = gath.at[where, pl.ds(part * half, half if part == 0 else planes - half)]
        pltpu.make_async_remote_copy(
            block, block, gath_send.at[part, before, at], gath_recv.at[part, gap],
            {"shift": lax.bitwise_xor(me, bit)}, device_id_type=MESH).wait_recv()

    def edge(plane, slot, to, to_slot):
        return pltpu.make_async_remote_copy(
            mext.at[0, plane], mext.at[0, slot], edge_send.at[to_slot], edge_recv.at[to_slot],
            {"dom": to}, device_id_type=MESH)

    edge_up = edge(planes, 0, lax.rem(dom + 1, doms), 0)
    edge_down = edge(1, planes + 1, lax.rem(dom + doms - 1, doms), 1)

    for at in range(2, 2 + half):
        moment(at)
    forward(0, 0)
    for at in range(2 + half, planes + 2):
        moment(at)
    forward(0, 1)

    def keep(gap):
        where = lax.bitwise_xor(me, gap)
        place = out.at[:, pl.ds(pl.multiple_of(where * cols, 8), cols), :] if sliced else out.at[where]
        return pltpu.make_async_copy(gath.at[where], place, out_sem.at[gap])

    keep(0).start()

    @pl.when(above)
    def _():
        edge_up.start()

    @pl.when(below)
    def _():
        edge_down.start()

    @pl.when(jnp.logical_not(below))
    def _():
        mext[0, 0] = jnp.zeros((cols, cells), jnp.float32)

    @pl.when(jnp.logical_not(above))
    def _():
        mext[0, planes + 1] = jnp.zeros((cols, cells), jnp.float32)

    @pl.when(below)
    def _():
        edge_up.wait_recv()
        edge_down.wait_send()

    @pl.when(above)
    def _():
        edge_down.wait_recv()
        edge_up.wait_send()

    def apply(at):
        get = field(mext, 0, at)
        values = []
        for tile in range(reps):
            onsite = 6.0 + jnp.broadcast_to(pe[at - 1 : at, lanes(tile)], (cols, LANES))
            values.append(onsite * get(0, tile) - neighbours(get, 0, tile, reps))
        for tile, value in enumerate(gather_back(values)):
            rhs[at - 1, :cols, lanes(tile)] = value

    for at in range(1, planes + 1):
        apply(at)

    arrivals = sorted(
        ((gap, part) for gap in range(1, count) for part in range(2)),
        key=lambda pair: (pair[0] & 1, bin(pair[0]).count("1"), last_of(pair[0], orders[pair[1]]), pair[1]))
    done = set()
    for gap, part in arrivals:
        arrived(gap, part)
        forward(gap, part)
        if (gap, 1 - part) in done:
            keep(gap).start()
        done.add((gap, part))

    def contract(at, value):
        left_hi, left_lo = split(rhs[at])
        right_hi, right_lo = split(gath[:, at].reshape(count * cols, cells))
        dims = (((1,), (1,)), ((), ()))
        dot = functools.partial(lax.dot_general, dimension_numbers=dims, preferred_element_type=jnp.float32)
        return value + (dot(left_hi, right_hi) + (dot(left_hi, right_lo) + dot(left_lo, right_hi)))

    value = lax.fori_loop(0, planes, contract, jnp.zeros((2 * cols, count * cols), jnp.float32))
    red[dom] = value
    to_all(red, red_send, red_recv, "dom", dom, doms)
    total = red[0]
    for other in range(1, doms):
        total = total + red[other]
    fin[me] = total * (1.0 / total_cells)
    to_all(fin, fin_send, fin_recv, "shift", me, count)

    out_h[...] = fin[:, :cols].reshape(count * cols, count * cols)
    out_b[...] = fin[:, cols:].reshape(count * cols, count * cols)
    for gap in range(count):
        keep(gap).wait()
    for part in range(2):
        for gap in range(count):
            for at in range(last_of(gap, orders[part]) + 1, len(bits)):
                hop(gap, part, at).wait_send()


def on_device(count, doms, samples, potential):
    planes, vectors, cells = samples.shape
    own = vectors // count
    cols = -(-own // 8) * 8
    sliced = own == cols
    if not sliced:
        part = lax.dynamic_slice_in_dim(samples, lax.axis_index("shift") * own, own, axis=1)
        samples = jnp.pad(part, ((0, 0), (0, cols - own), (0, 0)))
    width = -(-count * 8 // LANES) * LANES
    levels = count.bit_length() - 1
    f32 = jnp.float32
    dma = pltpu.SemaphoreType.DMA
    vmem = pl.BlockSpec(memory_space=pltpu.VMEM)
    size = count * cols
    shape = (planes, vectors, cells) if sliced else (count, planes, cols, cells)
    subspace, reduced_h, reduced_b = pl.pallas_call(
        functools.partial(kernel, count, doms, sliced, planes * doms * cells),
        out_shape=(
            jax.ShapeDtypeStruct(shape, f32),
            jax.ShapeDtypeStruct((size, size), f32),
            jax.ShapeDtypeStruct((size, size), f32),
        ),
        in_specs=[pl.BlockSpec(memory_space=pl.ANY), vmem],
        out_specs=(pl.BlockSpec(memory_space=pl.ANY), vmem, vmem),
        scratch_shapes=[
            pltpu.VMEM((count, planes, cols, cells), f32),
            pltpu.VMEM((count, 2 * cols, size), f32),
            pltpu.VMEM((planes + 4, cols, cells), f32),
            pltpu.VMEM((planes + 4, cols, cells), f32),
            pltpu.VMEM((2, planes, cells), f32),
            pltpu.VMEM((planes + 4, cells), f32),
            pltpu.VMEM((count, 2, planes + 4, cells), f32),
            pltpu.VMEM((count, 2, planes + 4, cells), f32),
            pltpu.VMEM((count, 2, planes + 4, cols, cells), f32),
            pltpu.VMEM((count, 2, planes + 4, cols, cells), f32),
            pltpu.VMEM((count, 2, planes + 4, cols, cells), f32),
            pltpu.VMEM((doms, cols, width), f32),
            pltpu.VMEM((count, 4, cols, LANES), f32),
            pltpu.VMEM((1, planes + 2, cols, cells), f32),
            pltpu.VMEM((planes, 2 * cols, cells), f32),
            pltpu.VMEM((doms, 2 * cols, count * cols), f32),
            dma,
            dma((2, 2)), dma((2, 2)),
            dma((doms,)), dma((doms,)),
            dma((2,)), dma((2,)),
            dma((2, count, levels)), dma((2, count)), dma((count,)),
            dma((doms,)), dma((doms,)),
            dma((count,)), dma((count,)),
        ],
        compiler_params=pltpu.CompilerParams(
            collective_id=0, has_side_effects=True, vmem_limit_bytes=56 * 1024 * 1024
        ),
        name="feast_step",
    )(samples, potential)
    if sliced:
        return subspace, reduced_h, reduced_b
    subspace = jnp.transpose(subspace[:, :, :own], (1, 0, 2, 3)).reshape(planes, vectors, cells)

    def trim(value):
        return value.reshape(count, cols, count, cols)[:, :own, :, :own].reshape(vectors, vectors)

    return subspace, trim(reduced_h), trim(reduced_b)


def solution(mesh):
    in_specs = (P("dom", None, None), P("dom", None))
    out_specs = (P("dom", None, None), P(), P())
    return jax.shard_map(
        functools.partial(on_device, mesh.shape["shift"], mesh.shape["dom"]),
        mesh=mesh, in_specs=in_specs, out_specs=out_specs, check_vma=False,
    )
```

```python
import functools
import math

import jax
import jax.numpy as jnp
from jax import lax
from jax.experimental import pallas as pl
from jax.experimental.pallas import tpu as pltpu
from jax.sharding import PartitionSpec as P

NX = 32
NY = 32
LANES = 128

CENTRE = 3.0
RADIUS = 2.0
RIDGE = 0.01
MESH = pl.DeviceIdType.MESH


def tiles_of(value):
    return [value[:, at : at + LANES] for at in range(0, value.shape[1], LANES)]


def lane_of(value):
    return lax.broadcasted_iota(jnp.int32, value.shape, 1)


def spread(tiles):
    count, per = len(tiles), LANES // NY
    block = lane_of(tiles[0]) // NY
    out = []
    for at in range(count):
        for to in range(per):
            x = to * count + at
            part = tiles[x // per]
            move = (NY * (to - x % per)) % LANES
            part = pltpu.roll(part, move, 1) if move else part
            value = part if to == 0 else jnp.where(block == to, part, value)
        out.append(value)
    return out


def gather_back(tiles):
    count, per = len(tiles), LANES // NY
    block = lane_of(tiles[0]) // NY
    out = []
    for at in range(count):
        for to in range(per):
            x = at * per + to
            part = tiles[x % count]
            move = (NY * (to - x // count)) % LANES
            part = pltpu.roll(part, move, 1) if move else part
            value = part if to == 0 else jnp.where(block == to, part, value)
        out.append(value)
    return out


def neighbours(get, at, tile, count):
    here = get(at, tile)
    lane = lane_of(here)
    column = lane % NY
    low = jnp.where(column != 0, pltpu.roll(here, 1, 1), 0.0)
    high = jnp.where(column != NY - 1, pltpu.roll(here, LANES - 1, 1), 0.0)
    if tile > 0:
        left = get(at, tile - 1)
    else:
        left = jnp.where(lane >= NY, pltpu.roll(get(at, count - 1), NY, 1), 0.0)
    if tile < count - 1:
        right = get(at, tile + 1)
    else:
        right = jnp.where(lane < LANES - NY, pltpu.roll(get(at, 0), LANES - NY, 1), 0.0)
    return ((low + high) + (left + right)) + (get(at - 1, tile) + get(at + 1, tile))


def split(value):
    high = value.astype(jnp.bfloat16)
    return high, (value - high.astype(jnp.float32)).astype(jnp.bfloat16)


def kernel(
    count, doms, sliced, total_cells,
    samples, pot, out, out_h, out_b,
    gath, fin,
    sraw, sext, pot_near, pe, inv, wd, ua, ub, p1, gram, coef, mext, rhs, red,
    local_sem, halo_send, halo_recv, gram_send, gram_recv, edge_send, edge_recv,
    gath_send, gath_recv, out_sem, red_send, red_recv, fin_send, fin_recv,
):
    me = lax.axis_index("shift")
    dom = lax.axis_index("dom")
    planes = pot.shape[0]
    cols, cells = sext.shape[1:]
    reps = cells // LANES
    below, above = dom > 0, dom < doms - 1

    def lanes(tile):
        return pl.ds(tile * LANES, LANES)


    barrier = pltpu.get_barrier_semaphore()
    for step in range(1, count):
        pl.semaphore_signal(barrier, inc=1, device_id={"shift": lax.rem(me + step, count)}, device_id_type=MESH)
    for step in range(1, doms):
        pl.semaphore_signal(barrier, inc=1, device_id={"dom": lax.rem(dom + step, doms)}, device_id_type=MESH)

    mine = pl.ds(pl.multiple_of(me * cols, 8), cols) if sliced else pl.ds(0, cols)
    own = pltpu.make_async_copy(samples.at[:, mine, :], sraw.at[pl.ds(2, planes)], local_sem)
    own.start()
    pl.semaphore_wait(barrier, count - 1 + doms - 1)

    def halo(first, slot, to, to_slot):
        return (
            pltpu.make_async_remote_copy(
                samples.at[pl.ds(first, 2), mine, :], sraw.at[pl.ds(slot, 2)],
                halo_send.at[to_slot, 0], halo_recv.at[to_slot, 0], {"dom": to}, device_id_type=MESH),
            pltpu.make_async_remote_copy(
                pot, pot_near.at[to_slot],
                halo_send.at[to_slot, 1], halo_recv.at[to_slot, 1], {"dom": to}, device_id_type=MESH),
        )

    up = halo(planes - 2, 0, lax.rem(dom + 1, doms), 0)
    down = halo(0, planes + 2, lax.rem(dom + doms - 1, doms), 1)

    @pl.when(above)
    def _():
        for copy in up:
            copy.start()

    @pl.when(below)
    def _():
        for copy in down:
            copy.start()

    @pl.when(jnp.logical_not(below))
    def _():
        sraw[0:2] = jnp.zeros((2, cols, cells), jnp.float32)
        pot_near[0] = jnp.zeros((planes, cells), jnp.float32)

    @pl.when(jnp.logical_not(above))
    def _():
        sraw[planes + 2 : planes + 4] = jnp.zeros((2, cols, cells), jnp.float32)
        pot_near[1] = jnp.zeros((planes, cells), jnp.float32)

    def row_at(at):
        if at < 2:
            return planes + at
        return at - 2 if at < planes + 2 else at

    def diagonals(rows):
        for tile, value in enumerate(spread(tiles_of(pe[rows]))):
            pe[rows, lanes(tile)] = value
        for node in range(count):
            angle = math.pi * (node + 0.5) / count
            cos, sin = RADIUS * math.cos(angle), RADIUS * math.sin(angle)
            diag = (CENTRE + cos) - (6.0 + pe[rows])
            over = 1.0 / (diag * diag + sin * sin)
            inv_re, inv_im = diag * over, -sin * over
            inv[node, 0, rows] = inv_re
            inv[node, 1, rows] = inv_im
            wd[node, 0, rows] = (cos / count) * inv_re - (sin / count) * inv_im
            wd[node, 1, rows] = (cos / count) * inv_im + (sin / count) * inv_re

    def spread_plane(at, carry):
        for tile, value in enumerate(spread(tiles_of(sraw[at]))):
            sext[at, :, lanes(tile)] = value
        return carry

    pe[0:planes] = pot[...]
    diagonals(slice(0, planes))
    own.wait()
    lax.fori_loop(2, planes + 2, spread_plane, 0)

    width = gram.shape[2]
    lane_at = lax.broadcasted_iota(jnp.int32, (cols, width), 1)

    def row(ref, node, part, at, tile):
        return jnp.broadcast_to(ref[node, part, row_at(at) : row_at(at) + 1, lanes(tile)], (cols, LANES))

    def field(ref, part, centre):
        seen = {}

        def get(shift, tile):
            if (shift, tile) not in seen:
                seen[shift, tile] = ref[part, centre + shift, :, lanes(tile)]
            return seen[shift, tile]

        return get

    edge_planes = (1, 2, planes + 1, planes + 2)

    def inner(node, carry):
        one_node(node, range(2, planes + 2), range(3, planes + 1))
        return carry

    def one_node(node, firsts, seconds):
        def first(at):
            for tile in range(reps):
                s = sext[at, :, lanes(tile)]
                ua[node, 0, at, :, lanes(tile)] = s * row(inv, node, 0, at, tile)
                ua[node, 1, at, :, lanes(tile)] = s * row(inv, node, 1, at, tile)


        def second(at):
            u_re, u_im = field(ua.at[node], 0, at), field(ua.at[node], 1, at)
            for tile in range(reps):
                p_re = sext[at, :, lanes(tile)] + neighbours(u_re, 0, tile, reps)
                p_im = neighbours(u_im, 0, tile, reps)
                p1[node, 0, at, :, lanes(tile)] = p_re
                p1[node, 1, at, :, lanes(tile)] = p_im
                i_re, i_im = row(inv, node, 0, at, tile), row(inv, node, 1, at, tile)
                ub[node, 0, at, :, lanes(tile)] = p_re * i_re - p_im * i_im
                ub[node, 1, at, :, lanes(tile)] = p_re * i_im + p_im * i_re

        for at in firsts:
            first(at)
        for at in seconds:
            second(at)

    lax.fori_loop(0, count, inner, 0)

    @pl.when(below)
    def _():
        for copy in up:
            copy.wait_recv()
        for copy in down:
            copy.wait_send()

    @pl.when(above)
    def _():
        for copy in down:
            copy.wait_recv()
        for copy in up:
            copy.wait_send()

    pe[planes : planes + 2] = pot_near[0, planes - 2 : planes]
    pe[planes + 2 : planes + 4] = pot_near[1, 0:2]
    diagonals(slice(planes, planes + 4))
    for at in (0, 1, planes + 2, planes + 3):
        spread_plane(at, 0)

    def each_node(node, packed):
        one_node(node, (0, 1, planes + 2, planes + 3), edge_planes)

        @pl.when(jnp.logical_not(below))
        def _():
            ub[node, 0, 1] = jnp.zeros((cols, cells), jnp.float32)
            ub[node, 1, 1] = jnp.zeros((cols, cells), jnp.float32)

        @pl.when(jnp.logical_not(above))
        def _():
            ub[node, 0, planes + 2] = jnp.zeros((cols, cells), jnp.float32)
            ub[node, 1, planes + 2] = jnp.zeros((cols, cells), jnp.float32)

        def third(at, sums):
            u_re, u_im = field(ub.at[node], 0, at), field(ub.at[node], 1, at)
            for tile in range(reps):
                s = sext[at, :, lanes(tile)]
                a_re, a_im = p1[node, 0, at, :, lanes(tile)], p1[node, 1, at, :, lanes(tile)]
                b_re = a_re + neighbours(u_re, 0, tile, reps)
                b_im = a_im + neighbours(u_im, 0, tile, reps)
                terms = (
                    a_re * a_re + a_im * a_im, a_re * s, -(a_im * s),
                    a_re * b_re + a_im * b_im, a_re * b_im - a_im * b_re,
                    b_re * b_re + b_im * b_im, b_re * s, -(b_im * s),
                )
                sums = tuple(old + term for old, term in zip(sums, terms))
            return sums

        zero = jnp.zeros((cols, LANES), jnp.float32)
        sums = lax.fori_loop(2, planes + 2, third, (zero,) * 8)
        for at, value in enumerate(sums):
            packed = jnp.where(lane_at == node * 8 + at, jnp.sum(value, axis=1, keepdims=True), packed)
        return packed

    gram[dom] = lax.fori_loop(0, count, each_node, jnp.zeros((cols, width), jnp.float32))

    def to_all(buffer, sends, recvs, axis, place, size):
        out = [
            pltpu.make_async_remote_copy(
                buffer.at[place], buffer.at[place], sends.at[step - 1], recvs.at[step - 1],
                {axis: lax.rem(place + step, size)}, device_id_type=MESH)
            for step in range(1, size)
        ]
        for copy in out:
            copy.start()
        for copy in out:
            copy.wait()

    to_all(gram, gram_send, gram_recv, "dom", dom, doms)
    total = gram[0]
    for other in range(1, doms):
        total = total + gram[other]
    g_one, q_one_re, q_one_im, g_mix_re, g_mix_im, g_two, q_two_re, q_two_im = [
        total if at == 0 else pltpu.roll(total, width - at, 1) for at in range(8)
    ]
    ridge = RIDGE * (g_one + g_two) / 2.0
    determ = (g_one + ridge) * (g_two + ridge) - (g_mix_re * g_mix_re + g_mix_im * g_mix_im)
    coefs = (
        ((g_two + ridge) * q_one_re - (g_mix_re * q_two_re - g_mix_im * q_two_im)) / determ,
        ((g_two + ridge) * q_one_im - (g_mix_re * q_two_im + g_mix_im * q_two_re)) / determ,
        ((g_one + ridge) * q_two_re - (g_mix_re * q_one_re + g_mix_im * q_one_im)) / determ,
        ((g_one + ridge) * q_two_im - (g_mix_re * q_one_im - g_mix_im * q_one_re)) / determ,
    )
    for node in range(count):
        for at, value in enumerate(coefs):
            coef[node, at] = jnp.broadcast_to(value[:, node * 8 : node * 8 + 1], (cols, LANES))

    def moment(at):
        values = [jnp.zeros((cols, LANES), jnp.float32)] * reps
        for node in range(count):
            c1r, c1i, c2r, c2i = [coef[node, part] for part in range(4)]
            for tile in range(reps):
                s = sext[at, :, lanes(tile)]
                a_re, a_im = p1[node, 0, at, :, lanes(tile)], p1[node, 1, at, :, lanes(tile)]
                y_re = c1r * s + (c2r * a_re - c2i * a_im)
                y_im = c1i * s + (c2r * a_im + c2i * a_re)
                values[tile] = values[tile] + (
                    row(wd, node, 0, at, tile) * y_re - row(wd, node, 1, at, tile) * y_im)
        for tile, value in enumerate(values):
            mext[0, at - 1, :, lanes(tile)] = value
        for tile, value in enumerate(gather_back(values)):
            gath[me, at - 2, :, lanes(tile)] = value
            rhs[at - 2, cols:, lanes(tile)] = value


    bits = [1 << at for at in range(count.bit_length() - 1)]
    orders = [bits[1:] + bits[:1], bits[1:][::-1] + bits[:1]]
    half = planes // 2

    def last_of(gap, order):
        return max([at for at, bit in enumerate(order) if gap & bit], default=-1)

    def hop(gap, part, at):
        bit = orders[part][at]
        where = lax.bitwise_xor(me, gap)
        block = gath.at[where, pl.ds(part * half, half if part == 0 else planes - half)]
        return pltpu.make_async_remote_copy(
            block, block, gath_send.at[part, gap, at], gath_recv.at[part, gap | bit],
            {"shift": lax.bitwise_xor(me, bit)}, device_id_type=MESH)

    def forward(gap, part, only=None):
        for at in range(last_of(gap, orders[part]) + 1, len(bits)):
            hop(gap, part, at).start()

    def arrived(gap, part):
        at = last_of(gap, orders[part])
        before = gap & ~orders[part][at]
        bit = orders[part][at]
        where = lax.bitwise_xor(me, gap)
        block = gath.at[where, pl.ds(part * half, half if part == 0 else planes - half)]
        pltpu.make_async_remote_copy(
            block, block, gath_send.at[part, before, at], gath_recv.at[part, gap],
            {"shift": lax.bitwise_xor(me, bit)}, device_id_type=MESH).wait_recv()

    def edge(plane, slot, to, to_slot):
        return pltpu.make_async_remote_copy(
            mext.at[0, plane], mext.at[0, slot], edge_send.at[to_slot], edge_recv.at[to_slot],
            {"dom": to}, device_id_type=MESH)

    edge_up = edge(planes, 0, lax.rem(dom + 1, doms), 0)
    edge_down = edge(1, planes + 1, lax.rem(dom + doms - 1, doms), 1)

    for at in range(2, 2 + half):
        moment(at)
    forward(0, 0)
    for at in range(2 + half, planes + 2):
        moment(at)
    forward(0, 1)

    def keep(gap):
        where = lax.bitwise_xor(me, gap)
        place = out.at[:, pl.ds(pl.multiple_of(where * cols, 8), cols), :] if sliced else out.at[where]
        return pltpu.make_async_copy(gath.at[where], place, out_sem.at[gap])

    keep(0).start()

    @pl.when(above)
    def _():
        edge_up.start()

    @pl.when(below)
    def _():
        edge_down.start()

    @pl.when(jnp.logical_not(below))
    def _():
        mext[0, 0] = jnp.zeros((cols, cells), jnp.float32)

    @pl.when(jnp.logical_not(above))
    def _():
        mext[0, planes + 1] = jnp.zeros((cols, cells), jnp.float32)

    @pl.when(below)
    def _():
        edge_up.wait_recv()
        edge_down.wait_send()

    @pl.when(above)
    def _():
        edge_down.wait_recv()
        edge_up.wait_send()

    def apply(at):
        get = field(mext, 0, at)
        values = []
        for tile in range(reps):
            onsite = 6.0 + jnp.broadcast_to(pe[at - 1 : at, lanes(tile)], (cols, LANES))
            values.append(onsite * get(0, tile) - neighbours(get, 0, tile, reps))
        for tile, value in enumerate(gather_back(values)):
            rhs[at - 1, :cols, lanes(tile)] = value

    for at in range(1, planes + 1):
        apply(at)

    arrivals = sorted(
        ((gap, part) for gap in range(1, count) for part in range(2)),
        key=lambda pair: (pair[0] & 1, bin(pair[0]).count("1"), last_of(pair[0], orders[pair[1]]), pair[1]))
    done = set()
    for gap, part in arrivals:
        arrived(gap, part)
        forward(gap, part)
        if (gap, 1 - part) in done:
            keep(gap).start()
        done.add((gap, part))

    def contract(at, value):
        left_hi, left_lo = split(rhs[at])
        right_hi, right_lo = split(gath[:, at].reshape(count * cols, cells))
        dims = (((1,), (1,)), ((), ()))
        dot = functools.partial(lax.dot_general, dimension_numbers=dims, preferred_element_type=jnp.float32)
        return value + (dot(left_hi, right_hi) + (dot(left_hi, right_lo) + dot(left_lo, right_hi)))

    value = lax.fori_loop(0, planes, contract, jnp.zeros((2 * cols, count * cols), jnp.float32))
    red[dom] = value
    to_all(red, red_send, red_recv, "dom", dom, doms)
    total = red[0]
    for other in range(1, doms):
        total = total + red[other]
    fin[me] = total * (1.0 / total_cells)
    to_all(fin, fin_send, fin_recv, "shift", me, count)

    out_h[...] = fin[:, :cols].reshape(count * cols, count * cols)
    out_b[...] = fin[:, cols:].reshape(count * cols, count * cols)
    for gap in range(count):
        keep(gap).wait()
    for part in range(2):
        for gap in range(count):
            for at in range(last_of(gap, orders[part]) + 1, len(bits)):
                hop(gap, part, at).wait_send()


def on_device(count, doms, samples, potential):
    planes, vectors, cells = samples.shape
    own = vectors // count
    cols = -(-own // 8) * 8
    sliced = own == cols
    if not sliced:
        part = lax.dynamic_slice_in_dim(samples, lax.axis_index("shift") * own, own, axis=1)
        samples = jnp.pad(part, ((0, 0), (0, cols - own), (0, 0)))
    width = -(-count * 8 // LANES) * LANES
    levels = count.bit_length() - 1
    f32 = jnp.float32
    dma = pltpu.SemaphoreType.DMA
    vmem = pl.BlockSpec(memory_space=pltpu.VMEM)
    plane = cols * cells * 4
    held = 6 * count * (planes + 4) * plane + 4 * count * (planes + 16) * cells * 4
    held += (count + 10) * (planes + 4) * plane
    size = count * cols
    shape = (planes, vectors, cells) if sliced else (count, planes, cols, cells)
    subspace, reduced_h, reduced_b = pl.pallas_call(
        functools.partial(kernel, count, doms, sliced, planes * doms * cells),
        out_shape=(
            jax.ShapeDtypeStruct(shape, f32),
            jax.ShapeDtypeStruct((size, size), f32),
            jax.ShapeDtypeStruct((size, size), f32),
        ),
        in_specs=[pl.BlockSpec(memory_space=pltpu.HBM), vmem],
        out_specs=(pl.BlockSpec(memory_space=pl.ANY), vmem, vmem),
        scratch_shapes=[
            pltpu.VMEM((count, planes, cols, cells), f32),
            pltpu.VMEM((count, 2 * cols, size), f32),
            pltpu.VMEM((planes + 4, cols, cells), f32),
            pltpu.VMEM((planes + 4, cols, cells), f32),
            pltpu.VMEM((2, planes, cells), f32),
            pltpu.VMEM((planes + 4, cells), f32),
            pltpu.VMEM((count, 2, planes + 4, cells), f32),
            pltpu.VMEM((count, 2, planes + 4, cells), f32),
            pltpu.VMEM((count, 2, planes + 4, cols, cells), f32),
            pltpu.VMEM((count, 2, planes + 4, cols, cells), f32),
            pltpu.VMEM((count, 2, planes + 4, cols, cells), f32),
            pltpu.VMEM((doms, cols, width), f32),
            pltpu.VMEM((count, 4, cols, LANES), f32),
            pltpu.VMEM((1, planes + 2, cols, cells), f32),
            pltpu.VMEM((planes, 2 * cols, cells), f32),
            pltpu.VMEM((doms, 2 * cols, count * cols), f32),
            dma,
            dma((2, 2)), dma((2, 2)),
            dma((doms,)), dma((doms,)),
            dma((2,)), dma((2,)),
            dma((2, count, levels)), dma((2, count)), dma((count,)),
            dma((doms,)), dma((doms,)),
            dma((count,)), dma((count,)),
        ],
        compiler_params=pltpu.CompilerParams(
            collective_id=0, has_side_effects=True, vmem_limit_bytes=min(held + 2 * 1024 * 1024, 60 * 1024 * 1024)
        ),
        name="feast_step",
    )(samples, potential)
    if sliced:
        return subspace, reduced_h, reduced_b
    subspace = jnp.transpose(subspace[:, :, :own], (1, 0, 2, 3)).reshape(planes, vectors, cells)

    def trim(value):
        return value.reshape(count, cols, count, cols)[:, :own, :, :own].reshape(vectors, vectors)

    return subspace, trim(reduced_h), trim(reduced_b)


def solution(mesh):
    in_specs = (P("dom", None, None), P("dom", None))
    out_specs = (P("dom", None, None), P(), P())
    return jax.shard_map(
        functools.partial(on_device, mesh.shape["shift"], mesh.shape["dom"]),
        mesh=mesh, in_specs=in_specs, out_specs=out_specs, check_vma=False,
    )
```
